256 devices in a mesh: vocab: 32 (over z_lo, x, core), seq: 8 (over y, z_hi).
Axes of the slice: x: 4, y: 4, z: 8 (z_hi: 2, z_lo: 4; z = z_hi * 4 + z_lo), core: 2. Of those that a mesh axis runs over, the one named last changes fastest.
Arguments:
- hidden_states: bfloat16 [2048, 3584], P('seq', 'vocab'), may hold values from -6 to 6
- norm_gain: float32 [3584], replicated, may hold values from 0.5 to 1.5
- embedding: bfloat16 [256000, 3584], P(('vocab', 'seq')), may hold values from -0.29882812 to 0.29882812
- targets: int32 [2048], replicated, may hold values from 0 to 255999
Outputs:
- token_loss: float32 [2048], P('seq')
- mean_loss: float32 [], replicated
The draws below stay inside these ranges and needn't reach their ends.
All inputs are finite; a program needn't handle non-finite values.
Results may differ from the reference program's by a relative error of at most 0.0005.
Values may be sent and summed in bfloat16 or wider, within the bound.
No kernel may reach another device: no remote copies, remote signals or barrier semaphores. Data moves between devices by JAX's collectives and lax.ppermute only.
A program may use at most 64 MiB of HBM per device.

```python
import jax
import jax.numpy as jnp
from jax import lax

D = 3584
VOCAB = 256000
TOKENS = 2048
N_VOCAB = 32


def place_ends(values, own_key, smallest, largest):
    longest = values.shape.index(max(values.shape))
    spots = []
    for shift in (0, 1):
        where = [jax.random.randint(jax.random.fold_in(own_key, axis), (), 0, length) for axis, length in enumerate(values.shape)]
        where[longest] = (where[longest] + shift) % values.shape[longest]
        spots.append(tuple(where))
    return values.at[spots[0]].set(smallest).at[spots[1]].set(largest)


def block_scale(key, shape, cuts, least, high):
    def one(dim, blocks):
        steps = jax.random.uniform(jax.random.fold_in(jax.random.fold_in(key, 6), dim), (blocks,), jnp.float32, least / len(cuts), high / len(cuts))
        return jnp.repeat(jnp.exp(steps), shape[dim] // blocks).reshape((-1,) + (1,) * (len(shape) - dim - 1))

    level = one(*cuts[0])
    for cut in cuts[1:]:
        level = level * one(*cut)
    return level


def scatter_about(rng, extent, deviation, reach, split=(), held_as=jnp.bfloat16):
    drawn = jax.random.normal(rng, extent, jnp.float32) * deviation
    if len(split) > 0:
        drawn = block_scale(rng, extent, split, -0.22, 0.18) * drawn
    return jnp.clip(drawn, min=-reach, max=reach).astype(held_as)


def setup_inputs(seed: int = 0) -> dict:
    seeds = jax.random.split(jax.random.key(seed), 5)
    return {
        "hidden_states": scatter_about(seeds[0], (TOKENS, D), 1.0, 6.0, ((0, 8), (1, 32))),
        "norm_gain": jnp.clip(1.0 + 0.1 * jax.random.normal(seeds[1], (D,), jnp.float32), 0.5, 1.5),
        "embedding": scatter_about(seeds[2], (VOCAB, D), (3.0 * D ** -0.5), 0.29882812, ((0, 256),)),
        "targets": place_ends(jax.random.randint(seeds[3], (TOKENS,), 0, VOCAB), jax.random.fold_in(seeds[3], 1), 0, VOCAB - 1).astype(jnp.int32),
    }


def reference(hidden_states, norm_gain, embedding, targets):
    values = hidden_states.astype(jnp.float32)
    meansq = lax.optimization_barrier(jnp.mean(values * values, axis=-1, keepdims=True))
    normed = (values * lax.rsqrt(meansq + 1e-06) * norm_gain).astype(jnp.bfloat16)
    block_rows = VOCAB // N_VOCAB
    blocks = embedding.reshape(N_VOCAB, block_rows, D)
    starts = jnp.arange(N_VOCAB, dtype=jnp.int32) * block_rows

    def visit(carry, inputs):
        total, picked = carry
        table, start = inputs
        scores = jnp.dot(table, normed.T, preferred_element_type=jnp.float32)
        capped = 30.0 * jnp.tanh(scores / 30.0)
        total = total + lax.optimization_barrier(jnp.sum(jnp.exp(capped), axis=0))
        ids = start + jnp.arange(block_rows, dtype=jnp.int32)
        hit = ids[:, None] == targets[None, :]
        picked = picked + lax.optimization_barrier(jnp.sum(jnp.where(hit, capped, 0.0), axis=0))
        return ((total, picked), None)
    zeros = jnp.zeros((TOKENS,), jnp.float32)
    (total, picked), unused = lax.scan(visit, (zeros, zeros), (blocks, starts))
    token_loss = jnp.log(total) - picked
    return (token_loss, jnp.mean(token_loss))
```

```python
import functools

import jax
import jax.numpy as jnp
import numpy as np
from jax import lax
from jax.experimental import pallas as pl
from jax.experimental.pallas import tpu as pltpu
from jax.sharding import Mesh
from jax.sharding import PartitionSpec as P

AXES = ("zlo", "x", "core", "y", "zhi")
VOCAB = ("zlo", "x", "core")
SEQ = ("y", "zhi")

EARLY = (("z4", 0), ("x", 0), ("y", 0), ("z", 0))
ORDERS = ("xyz", "yzx", "zxy")
CUTS = (0, 6, 11, 16)
ROWS = 8


def pair(p, which, n):
    return jnp.where(which == 0, p ^ 1, (((p + 1) % n) ^ 1) + n - 1) % n


def partner(dim, ab, x, y, z, c):
    w = c ^ ab
    if dim == "x":
        return pair(x, w, 4), y, z
    if dim == "y":
        return x, pair(y, w, 4), z
    if dim == "z":
        return x, y, pair(z, w, 8)
    return x, y, z ^ 4


def linear(x, y, z, c):
    return ((((z % 4) * 4 + x) * 2 + c) * 4 + y) * 2 + z // 4


@functools.lru_cache(None)
def stage_pairs(dim, ab):
    at = np.arange(256)
    zhi, y, c, x, zlo = at % 2, at // 2 % 4, at // 8 % 2, at // 16 % 4, at // 64
    z = zhi * 4 + zlo

    def ring(p, which, n):
        return np.where(which == 0, p ^ 1, (((p + 1) % n) ^ 1) + n - 1) % n

    w = c ^ ab
    if dim == "c":
        c = c ^ 1
    elif dim == "x":
        x = ring(x, w, 4)
    elif dim == "y":
        y = ring(y, w, 4)
    elif dim == "z":
        z = ring(z, w, 8)
    else:
        z = z ^ 4
    return tuple((int(a), int(b)) for a, b in zip(at, linear(x, y, z, c)))


def exchange(v, dim, ab):
    return lax.ppermute(v, AXES, stage_pairs(dim, ab))


def normalize(rows, norm_gain):
    values = rows.astype(jnp.float32)
    meansq = jnp.mean(values * values, axis=-1, keepdims=True)
    return (values * lax.rsqrt(meansq + 1e-06) * norm_gain).astype(jnp.bfloat16)


def score_kernel(tile, steps, base_ref, tgt_ref, *refs):
    *pieces, emb0, emb1, total_ref, picked_ref, rows, tot, pick, sems = refs
    step = pl.program_id(0)

    @pl.when(step == 0)
    def _():
        at, copies = 0, []
        for i, piece in enumerate(pieces):
            n = piece.shape[0]
            copies.append(pltpu.make_async_copy(piece, rows.at[pl.ds(at, n)], sems.at[i]))
            at += n
        for copy in copies:
            copy.start()
        tot[...] = jnp.zeros_like(tot)
        pick[...] = jnp.zeros_like(pick)
        for copy in copies:
            copy.wait()

    for which, emb in enumerate((emb0, emb1)):
        scores = lax.dot_general(
            emb[...], rows[...], (((1,), (1,)), ((), ())), preferred_element_type=jnp.float32
        )
        capped = 30.0 * jnp.tanh(scores * (1.0 / 30.0))
        grown = jnp.exp(capped)
        want = tgt_ref[...] - (base_ref[which] + step * tile)
        ids = lax.broadcasted_iota(jnp.int32, scores.shape, 0)
        hit = jnp.where(ids == want, capped, 0.0)
        wide = scores.shape[1]
        tot[...] += jnp.sum(grown.reshape(tile // 8, 8, wide), axis=0)
        pick[...] += jnp.sum(hit.reshape(tile // 8, 8, wide), axis=0)

    @pl.when(step == steps - 1)
    def _():
        total_ref[...] = jnp.sum(tot[...], axis=0, keepdims=True)
        picked_ref[...] = jnp.sum(pick[...], axis=0, keepdims=True)


def score(pieces, emb0, emb1, bases, tgt, tile=200):
    count, width = emb0.shape
    n = sum(p.shape[0] for p in pieces)
    steps = count // tile
    flat = pl.BlockSpec((1, n), lambda i, *_: (0, 0))
    table = pl.BlockSpec((tile, width), lambda i, *_: (i, 0))
    return pl.pallas_call(
        functools.partial(score_kernel, tile, steps),
        out_shape=[jax.ShapeDtypeStruct((1, n), jnp.float32)] * 2,
        grid_spec=pltpu.PrefetchScalarGridSpec(
            num_scalar_prefetch=1,
            grid=(steps,),
            in_specs=[flat] + [pl.BlockSpec(memory_space=pl.ANY)] * len(pieces) + [table] * 2,
            out_specs=[flat] * 2,
            scratch_shapes=[
                pltpu.VMEM((n, width), jnp.bfloat16),
                pltpu.VMEM((8, n), jnp.float32),
                pltpu.VMEM((8, n), jnp.float32),
                pltpu.SemaphoreType.DMA((len(pieces),)),
            ],
        ),
        compiler_params=pltpu.CompilerParams(
            dimension_semantics=("arbitrary",), vmem_limit_bytes=40 * 2**20
        ),
        cost_estimate=pl.CostEstimate(
            flops=4 * count * n * width,
            bytes_accessed=4 * count * width + 2 * n * width,
            transcendentals=4 * count * n,
        ),
        name="score",
    )(bases, tgt, *pieces, emb0, emb1)


def layout_of_rows():
    out = []
    for last in (0, 1):
        for k in range(3):
            for l2 in (0, 1):
                for l1 in (0, 1):
                    for e in range(CUTS[k], CUTS[k + 1]):
                        out.append((k, e, l1, l2, last))
    return np.array(out)


def sources():
    x, y, c = (lax.axis_index(a) for a in ("x", "y", "core"))
    z = lax.axis_index("zhi") * 4 + lax.axis_index("zlo")
    lay = layout_of_rows()
    n = len(lay)
    x, y, z = (jnp.full((n,), v, jnp.int32) for v in (x, y, z))

    def move(mask, dim, ab, x, y, z):
        mask = jnp.asarray(mask)
        return tuple(jnp.where(mask, a, b) for a, b in zip(partner(dim, ab, x, y, z, c), (x, y, z)))

    for s in (2, 1, 0):
        bit = lay[:, 2 + s] == 1
        dims = np.array([ORDERS[k][s] for k in lay[:, 0]])
        for dim in "xyz":
            x, y, z = move(bit & (dims == dim), dim, 1, x, y, z)
    for s in (3, 2, 1, 0):
        x, y, z = move((lay[:, 1] >> s) & 1 == 1, *EARLY[s], x, y, z)
    return x, y, z


def local(hidden_states, norm_gain, embedding, targets):
    all_count = targets.shape[0]
    block, part = hidden_states.shape
    core = lax.axis_index("core")
    y, zhi = lax.axis_index("y"), lax.axis_index("zhi")

    other = exchange(embedding, "c", 0)
    mine = ((lax.axis_index("zlo") * 4 + lax.axis_index("x")) * 2 * 8) + y * 2 + zhi
    bases = jnp.stack([mine + core * 8, mine + (1 - core) * 8]).astype(jnp.int32) * embedding.shape[0]

    sent = hidden_states.reshape(32, block // 32, part)
    came = lax.all_to_all(sent, VOCAB, split_axis=0, concat_axis=0, tiled=True)
    rows = jnp.moveaxis(came, 0, 1).reshape(block // 32, 32 * part)
    cur = normalize(rows, norm_gain)

    sx, sy, sz = sources()
    group = ((sy * 2 + sz // 4) * 4 + sz % 4) * 4 + sx
    tgt = jnp.take(targets.reshape(128, 2, ROWS), group, axis=0)
    tgt = jnp.where(core == 0, tgt[:, 0], tgt[:, 1]).reshape(2, 1, -1)

    for dim, ab in EARLY:
        cur = jnp.concatenate([cur, exchange(cur, dim, ab)], 0)
    groups = [cur[ROWS * a : ROWS * b] for a, b in zip(CUTS, CUTS[1:])]
    for s in (0, 1):
        groups = [jnp.concatenate([g, exchange(g, o[s], 1)], 0) for g, o in zip(groups, ORDERS)]
    arrived = [exchange(g, o[2], 1) for g, o in zip(groups, ORDERS)]

    first = score(groups, embedding, other, bases, tgt[0])
    second = score(arrived, embedding, other, bases, tgt[1])
    stats = jnp.stack([jnp.concatenate([a.reshape(-1, ROWS), b.reshape(-1, ROWS)]) for a, b in zip(first, second)])
    order = (group[None, :] == jnp.arange(128, dtype=jnp.int32)[:, None]).astype(jnp.float32)
    stats = jnp.einsum("gp,spi->sgi", order, stats, precision=lax.Precision.HIGHEST)

    flat = stats.reshape(1, 16, 128)
    got = lax.all_to_all(jnp.broadcast_to(flat, (32, 16, 128)), VOCAB, split_axis=0, concat_axis=0, tiled=True)
    summed = got.reshape(16, 2, 16, 128).sum(axis=0).reshape(1, 32, 128)
    got = lax.all_to_all(jnp.broadcast_to(summed, (8, 32, 128)), SEQ, split_axis=0, concat_axis=0, tiled=True)
    total, picked = jnp.moveaxis(got.sum(axis=0).reshape(2, 2, 128, ROWS), 1, 0)
    loss = jnp.log(total) - picked
    loss = jnp.moveaxis(loss, 0, 1).reshape(-1)
    token_loss = lax.dynamic_slice(loss, ((y * 2 + zhi) * block,), (block,))
    return token_loss, jnp.sum(loss) / all_count


def solution(mesh):
    torus = Mesh(mesh.devices.reshape(4, 4, 2, 4, 2), AXES)
    placed = (P(SEQ, VOCAB), P(), P(VOCAB + SEQ, None), P())
    return jax.shard_map(
        local, mesh=torus, in_specs=placed, out_specs=(P(SEQ), P()), check_vma=False
    )
```

```python
import functools

import jax
import jax.numpy as jnp
import numpy as np
from jax import lax
from jax.experimental import pallas as pl
from jax.experimental.pallas import tpu as pltpu
from jax.sharding import Mesh
from jax.sharding import PartitionSpec as P

AXES = ("zlo", "x", "core", "y", "zhi")
VOCAB = ("zlo", "x", "core")
SEQ = ("y", "zhi")

EARLY = (("z4", 0), ("x", 0), ("y", 0), ("z", 0))
ORDERS = ("xyz", "yzx", "zxy")
CUTS = (0, 6, 11, 16)
ROWS = 8
VMEM_LIMIT = 16 * 2**20


def pair(p, which, n):
    return jnp.where(which == 0, p ^ 1, (((p + 1) % n) ^ 1) + n - 1) % n


def partner(dim, ab, x, y, z, c):
    w = c ^ ab
    if dim == "x":
        return pair(x, w, 4), y, z
    if dim == "y":
        return x, pair(y, w, 4), z
    if dim == "z":
        return x, y, pair(z, w, 8)
    return x, y, z ^ 4


def linear(x, y, z, c):
    return ((((z % 4) * 4 + x) * 2 + c) * 4 + y) * 2 + z // 4


@functools.lru_cache(None)
def stage_pairs(dim, ab):
    at = np.arange(256)
    zhi, y, c, x, zlo = at % 2, at // 2 % 4, at // 8 % 2, at // 16 % 4, at // 64
    z = zhi * 4 + zlo

    def ring(p, which, n):
        return np.where(which == 0, p ^ 1, (((p + 1) % n) ^ 1) + n - 1) % n

    w = c ^ ab
    if dim == "c":
        c = c ^ 1
    elif dim == "x":
        x = ring(x, w, 4)
    elif dim == "y":
        y = ring(y, w, 4)
    elif dim == "z":
        z = ring(z, w, 8)
    else:
        z = z ^ 4
    return tuple((int(a), int(b)) for a, b in zip(at, linear(x, y, z, c)))


def exchange(v, dim, ab):
    return lax.ppermute(v, AXES, stage_pairs(dim, ab))


def normalize(rows, norm_gain):
    values = rows.astype(jnp.float32)
    meansq = jnp.mean(values * values, axis=-1, keepdims=True)
    return (values * lax.rsqrt(meansq + 1e-06) * norm_gain).astype(jnp.bfloat16)


def score_kernel(has_before, base_ref, tgt_ref, *refs):
    if has_before:
        before, *refs = refs
    *pieces, emb0, emb1, out_ref, rows, turned, tot, pick, sems = refs
    at, copies = 0, []
    for i, piece in enumerate(pieces):
        n = piece.shape[0]
        copies.append(pltpu.make_async_copy(piece, rows.at[pl.ds(at, n)], sems.at[i]))
        at += n
    for copy in copies:
        copy.start()
    tot[...] = jnp.zeros_like(tot)
    pick[...] = jnp.zeros_like(pick)
    for copy in copies:
        copy.wait()
    turned[...] = rows[...].T
    wide = turned.shape[1]
    for which, emb in enumerate((emb0, emb1)):
        count = emb.shape[0]
        for at in range(0, count, 256):
            tile = min(256, count - at)
            scores = jnp.dot(emb[at : at + tile], turned[...], preferred_element_type=jnp.float32)
            capped = 30.0 * jnp.tanh(scores * (1.0 / 30.0))
            grown = jnp.exp(capped)
            want = tgt_ref[...] - (base_ref[which] + at)
            ids = lax.broadcasted_iota(jnp.int32, scores.shape, 0)
            hit = jnp.where(ids == want, capped, 0.0)
            tot[...] += jnp.sum(grown.reshape(tile // 8, 8, wide), axis=0)
            pick[...] += jnp.sum(hit.reshape(tile // 8, 8, wide), axis=0)
    done = 0
    if has_before:
        done = before.shape[1]
        out_ref[:, :done] = before[...]
    out_ref[0:1, done:] = jnp.sum(tot[...], axis=0, keepdims=True)
    out_ref[1:2, done:] = jnp.sum(pick[...], axis=0, keepdims=True)


def score(pieces, emb0, emb1, bases, tgt, before=None):
    count, width = emb0.shape
    n = sum(p.shape[0] for p in pieces)
    vmem, anywhere = pl.BlockSpec(memory_space=pltpu.VMEM), pl.BlockSpec(memory_space=pl.ANY)
    earlier = [] if before is None else [before]
    return pl.pallas_call(
        functools.partial(score_kernel, len(earlier)),
        out_shape=jax.ShapeDtypeStruct((2, n + sum(b.shape[1] for b in earlier)), jnp.float32),
        in_specs=[pl.BlockSpec(memory_space=pltpu.SMEM)] + [vmem] * (1 + len(earlier)) + [anywhere] * len(pieces) + [vmem] * 2,
        out_specs=vmem,
        scratch_shapes=[
            pltpu.VMEM((n, width), jnp.bfloat16),
            pltpu.VMEM((width, n), jnp.bfloat16),
            pltpu.VMEM((8, n), jnp.float32),
            pltpu.VMEM((8, n), jnp.float32),
            pltpu.SemaphoreType.DMA((len(pieces),)),
        ],
        compiler_params=pltpu.CompilerParams(vmem_limit_bytes=VMEM_LIMIT),
        cost_estimate=pl.CostEstimate(
            flops=4 * count * n * width,
            bytes_accessed=4 * count * width + 2 * n * width,
            transcendentals=4 * count * n,
        ),
        name="score",
    )(bases, tgt, *earlier, *pieces, emb0, emb1)


def layout_of_rows():
    out = []
    for last in (0, 1):
        for k in range(3):
            for l2 in (0, 1):
                for l1 in (0, 1):
                    for e in range(CUTS[k], CUTS[k + 1]):
                        out.append((k, e, l1, l2, last))
    return np.array(out)


def sources():
    x, y, c = (lax.axis_index(a) for a in ("x", "y", "core"))
    z = lax.axis_index("zhi") * 4 + lax.axis_index("zlo")
    lay = layout_of_rows()
    n = len(lay)
    x, y, z = (jnp.full((n,), v, jnp.int32) for v in (x, y, z))

    def move(mask, dim, ab, x, y, z):
        mask = jnp.asarray(mask)
        return tuple(jnp.where(mask, a, b) for a, b in zip(partner(dim, ab, x, y, z, c), (x, y, z)))

    for s in (2, 1, 0):
        bit = lay[:, 2 + s] == 1
        dims = np.array([ORDERS[k][s] for k in lay[:, 0]])
        for dim in "xyz":
            x, y, z = move(bit & (dims == dim), dim, 1, x, y, z)
    for s in (3, 2, 1, 0):
        x, y, z = move((lay[:, 1] >> s) & 1 == 1, *EARLY[s], x, y, z)
    return x, y, z


def local(hidden_states, norm_gain, embedding, targets):
    all_count = targets.shape[0]
    block, part = hidden_states.shape
    core = lax.axis_index("core")
    y, zhi = lax.axis_index("y"), lax.axis_index("zhi")

    mine = ((lax.axis_index("zlo") * 4 + lax.axis_index("x")) * 2 * 8) + y * 2 + zhi
    bases = jnp.stack([mine + core * 8, mine + (1 - core) * 8]).astype(jnp.int32) * embedding.shape[0]

    sent = hidden_states.reshape(32, block // 32, part)
    came = lax.all_to_all(sent, VOCAB, split_axis=0, concat_axis=0, tiled=True)
    rows = jnp.moveaxis(came, 0, 1).reshape(block // 32, 32 * part)
    cur = normalize(rows, norm_gain)

    sx, sy, sz = sources()
    group = ((sy * 2 + sz // 4) * 4 + sz % 4) * 4 + sx
    tgt = jnp.take(targets.reshape(128, 2, ROWS), group, axis=0)
    tgt = jnp.where(core == 0, tgt[:, 0], tgt[:, 1]).reshape(2, 1, -1)
    tgt = [tgt[0], tgt[1]]

    cur, tgt, bases, embedding = lax.optimization_barrier((cur, tgt, bases, embedding))
    other = exchange(embedding, "c", 0)

    for dim, ab in EARLY:
        cur = jnp.concatenate([cur, exchange(cur, dim, ab)], 0)
    groups = [cur[ROWS * a : ROWS * b] for a, b in zip(CUTS, CUTS[1:])]
    for s in (0, 1):
        groups = [jnp.concatenate([g, exchange(g, o[s], 1)], 0) for g, o in zip(groups, ORDERS)]
    arrived = [exchange(g, o[2], 1) for g, o in zip(groups, ORDERS)]

    first = score(groups, embedding, other, bases, tgt[0])
    stats = score(arrived, embedding, other, bases, tgt[1], first).reshape(2, -1, ROWS)
    order = (group[None, :] == jnp.arange(128, dtype=jnp.int32)[:, None]).astype(jnp.float32)
    stats = jnp.einsum("gp,spi->sgi", order, stats, precision=lax.Precision.HIGHEST)

    flat = stats.reshape(1, 16, 128)
    got = lax.all_to_all(jnp.broadcast_to(flat, (32, 16, 128)), VOCAB, split_axis=0, concat_axis=0, tiled=True)
    summed = got.reshape(16, 2, 16, 128).sum(axis=0).reshape(1, 32, 128)
    got = lax.all_to_all(jnp.broadcast_to(summed, (8, 32, 128)), SEQ, split_axis=0, concat_axis=0, tiled=True)
    total, picked = jnp.moveaxis(got.sum(axis=0).reshape(2, 2, 128, ROWS), 1, 0)
    loss = jnp.log(total) - picked
    loss = jnp.moveaxis(loss, 0, 1).reshape(-1)
    token_loss = lax.dynamic_slice(loss, ((y * 2 + zhi) * block,), (block,))
    return token_loss, jnp.sum(loss) / all_count


def solution(mesh):
    torus = Mesh(mesh.devices.reshape(4, 4, 2, 4, 2), AXES)
    placed = (P(SEQ, VOCAB), P(), P(VOCAB + SEQ, None), P())
    return jax.shard_map(
        local, mesh=torus, in_specs=placed, out_specs=(P(SEQ), P()), check_vma=False
    )
```

```python
import functools

import jax
import jax.numpy as jnp
import numpy as np
from jax import lax
from jax.experimental import pallas as pl
from jax.experimental.pallas import tpu as pltpu
from jax.sharding import Mesh
from jax.sharding import PartitionSpec as P

AXES = ("zlo", "x", "core", "y", "zhi")
VOCAB = ("zlo", "x", "core")
SEQ = ("y", "zhi")

EARLY = (("z4", 0), ("x", 0), ("y", 0), ("z", 0))
ORDERS = ("xyz", "yzx", "zxy")
CUTS = (0, 7, 13, 16)
ROWS = 8
VMEM_LIMIT = 40 * 2**20


def pair(p, which, n):
    return jnp.where(which == 0, p ^ 1, (((p + 1) % n) ^ 1) + n - 1) % n


def partner(dim, ab, x, y, z, c):
    w = c ^ ab
    if dim == "x":
        return pair(x, w, 4), y, z
    if dim == "y":
        return x, pair(y, w, 4), z
    if dim == "z":
        return x, y, pair(z, w, 8)
    return x, y, z ^ 4


def linear(x, y, z, c):
    return ((((z % 4) * 4 + x) * 2 + c) * 4 + y) * 2 + z // 4


def stage_pairs(*stages):
    at = np.arange(256)
    zhi, y, c, x, zlo = at % 2, at // 2 % 4, at // 8 % 2, at // 16 % 4, at // 64
    z = zhi * 4 + zlo

    def ring(p, which, n):
        return np.where(which == 0, p ^ 1, (((p + 1) % n) ^ 1) + n - 1) % n

    for dim, ab in stages:
        w = c ^ ab
        if dim == "c":
            c = c ^ 1
        elif dim == "x":
            x = ring(x, w, 4)
        elif dim == "y":
            y = ring(y, w, 4)
        elif dim == "z":
            z = ring(z, w, 8)
        else:
            z = z ^ 4
    return tuple((int(a), int(b)) for a, b in zip(at, linear(x, y, z, c)))


def exchange(v, *stages):
    return lax.ppermute(v, AXES, stage_pairs(*stages))


def late(v, k, s):
    with jax.named_scope(f"late_{k}_{s}"):
        return exchange(v, (ORDERS[k][s], 1))


def normalize(rows, norm_gain):
    values = rows.astype(jnp.float32)
    meansq = jnp.mean(values * values, axis=-1, keepdims=True)
    return (values * lax.rsqrt(meansq + 1e-06) * norm_gain).astype(jnp.bfloat16)


def score_kernel(has_before, base_ref, tgt_ref, *refs):
    if has_before:
        before, *refs = refs
    *pieces, emb1, emb0, out_ref, rows, turned, own, tot, pick, sems = refs
    at, copies = 0, []
    for i, piece in enumerate(pieces):
        n = piece.shape[0]
        copies.append(pltpu.make_async_copy(piece, rows.at[pl.ds(at, n)], sems.at[i]))
        at += n
    copies.append(pltpu.make_async_copy(emb0, own, sems.at[len(pieces)]))
    for copy in copies:
        copy.start()
    tot[...] = jnp.zeros_like(tot)
    pick[...] = jnp.zeros_like(pick)
    for copy in copies[:-1]:
        copy.wait()
    turned[...] = rows[...].T
    wide = turned.shape[1]
    for which, emb in ((1, emb1), (0, own)):
        if which == 0:
            copies[-1].wait()
        count = emb.shape[0]
        for at in range(0, count, 256):
            tile = min(256, count - at)
            scores = jnp.dot(emb[at : at + tile], turned[...], preferred_element_type=jnp.float32)
            capped = 30.0 * jnp.tanh(scores * (1.0 / 30.0))
            grown = jnp.exp(capped)
            want = tgt_ref[...] - (base_ref[which] + at)
            ids = lax.broadcasted_iota(jnp.int32, scores.shape, 0)
            hit = jnp.where(ids == want, capped, 0.0)
            tot[...] += jnp.sum(grown.reshape(tile // 8, 8, wide), axis=0)
            pick[...] += jnp.sum(hit.reshape(tile // 8, 8, wide), axis=0)
    done = 0
    if has_before:
        done = before.shape[1]
        out_ref[:, :done] = before[...]
    out_ref[0:1, done:] = jnp.sum(tot[...], axis=0, keepdims=True)
    out_ref[1:2, done:] = jnp.sum(pick[...], axis=0, keepdims=True)


def score(pieces, emb0, emb1, bases, tgt, before=None):
    count, width = emb0.shape
    n = sum(p.shape[0] for p in pieces)
    vmem, anywhere = pl.BlockSpec(memory_space=pltpu.VMEM), pl.BlockSpec(memory_space=pl.ANY)
    earlier = [] if before is None else [before]
    return pl.pallas_call(
        functools.partial(score_kernel, len(earlier)),
        out_shape=jax.ShapeDtypeStruct((2, n + sum(b.shape[1] for b in earlier)), jnp.float32),
        in_specs=[pl.BlockSpec(memory_space=pltpu.SMEM)] + [vmem] * (1 + len(earlier)) + [anywhere] * len(pieces)
        + [vmem, pl.BlockSpec(memory_space=pltpu.HBM)],
        out_specs=vmem,
        scratch_shapes=[
            pltpu.VMEM((n, width), jnp.bfloat16),
            pltpu.VMEM((width, n), jnp.bfloat16),
            pltpu.VMEM((count, width), jnp.bfloat16),
            pltpu.VMEM((8, n), jnp.float32),
            pltpu.VMEM((8, n), jnp.float32),
            pltpu.SemaphoreType.DMA((len(pieces) + 1,)),
        ],
        compiler_params=pltpu.CompilerParams(vmem_limit_bytes=VMEM_LIMIT),
        cost_estimate=pl.CostEstimate(
            flops=4 * count * n * width,
            bytes_accessed=4 * count * width + 2 * n * width,
            transcendentals=4 * count * n,
        ),
        name="score",
    )(bases, tgt, *earlier, *pieces, emb1, emb0)


def layout_of_rows():
    out = []
    for last in (0, 1):
        for k in range(3):
            for l2 in (0, 1):
                for l1 in (0, 1):
                    for e in range(CUTS[k], CUTS[k + 1]):
                        out.append((k, e, l1, l2, last))
    return np.array(out)


def sources():
    x, y, c = (lax.axis_index(a) for a in ("x", "y", "core"))
    z = lax.axis_index("zhi") * 4 + lax.axis_index("zlo")
    lay = layout_of_rows()
    n = len(lay)
    x, y, z = (jnp.full((n,), v, jnp.int32) for v in (x, y, z))

    def move(mask, dim, ab, x, y, z):
        mask = jnp.asarray(mask)
        return tuple(jnp.where(mask, a, b) for a, b in zip(partner(dim, ab, x, y, z, c), (x, y, z)))

    for s in (2, 1, 0):
        bit = lay[:, 2 + s] == 1
        dims = np.array([ORDERS[k][s] for k in lay[:, 0]])
        for dim in "xyz":
            x, y, z = move(bit & (dims == dim), dim, 1, x, y, z)
    for s in (3, 2, 1, 0):
        x, y, z = move((lay[:, 1] >> s) & 1 == 1, *EARLY[s], x, y, z)
    return x, y, z


def local(hidden_states, norm_gain, embedding, targets):
    all_count = targets.shape[0]
    block, part = hidden_states.shape
    core = lax.axis_index("core")
    y, zhi = lax.axis_index("y"), lax.axis_index("zhi")

    mine = ((lax.axis_index("zlo") * 4 + lax.axis_index("x")) * 2 * 8) + y * 2 + zhi
    bases = jnp.stack([mine + core * 8, mine + (1 - core) * 8]).astype(jnp.int32) * embedding.shape[0]

    sent = hidden_states.reshape(32, block // 32, part)
    came = lax.all_to_all(sent, VOCAB, split_axis=0, concat_axis=0, tiled=True)
    rows = jnp.moveaxis(came, 0, 1).reshape(block // 32, 32 * part)
    cur = normalize(rows, norm_gain)

    sx, sy, sz = sources()
    group = ((sy * 2 + sz // 4) * 4 + sz % 4) * 4 + sx
    tgt = jnp.take(targets.reshape(128, 2, ROWS), group, axis=0)
    tgt = jnp.where(core == 0, tgt[:, 0], tgt[:, 1]).reshape(2, 1, -1)
    tgt = [tgt[0], tgt[1]]

    cur, tgt, bases, embedding = lax.optimization_barrier((cur, tgt, bases, embedding))
    other = exchange(embedding, ("c", 0))

    for a, b in (EARLY[:2], EARLY[2:]):
        cur = jnp.concatenate([cur, exchange(cur, a), exchange(cur, b), exchange(cur, a, b)], 0)
    groups = [cur[ROWS * a : ROWS * b] for a, b in zip(CUTS, CUTS[1:])]
    for s in (0, 1):
        groups = [jnp.concatenate([g, late(g, k, s)], 0) for k, g in enumerate(groups)]
    arrived = [late(g, k, 2) for k, g in enumerate(groups)]

    first = score(groups, embedding, other, bases, tgt[0])
    stats = score(arrived, embedding, other, bases, tgt[1], first).reshape(2, -1, ROWS)
    order = (group[None, :] == jnp.arange(128, dtype=jnp.int32)[:, None]).astype(jnp.float32)
    stats = jnp.einsum("gp,spi->sgi", order, stats, precision=lax.Precision.HIGHEST)

    flat = jnp.broadcast_to(stats.reshape(1, 16, 128), (16, 16, 128))
    summed = lax.all_to_all(flat, VOCAB[:2], split_axis=0, concat_axis=0, tiled=True).sum(axis=0, keepdims=True)
    flat = jnp.broadcast_to(summed, (16, 16, 128))
    got = lax.all_to_all(flat, VOCAB[2:] + SEQ, split_axis=0, concat_axis=0, tiled=True)
    total, picked = jnp.moveaxis(got.reshape(2, 8, 2, 128, ROWS).sum(axis=1), 1, 0)
    loss = jnp.log(total) - picked
    loss = jnp.moveaxis(loss, 0, 1).reshape(-1)
    token_loss = lax.dynamic_slice(loss, ((y * 2 + zhi) * block,), (block,))
    return token_loss, jnp.sum(loss) / all_count


def solution(mesh):
    torus = Mesh(mesh.devices.reshape(4, 4, 2, 4, 2), AXES)
    placed = (P(SEQ, VOCAB), P(), P(VOCAB + SEQ, None), P())
    return jax.shard_map(
        local, mesh=torus, in_specs=placed, out_specs=(P(SEQ), P()), check_vma=False
    )
```

```python
import functools

import jax
import jax.numpy as jnp
import numpy as np
from jax import lax
from jax.experimental import pallas as pl
from jax.experimental.pallas import tpu as pltpu
from jax.sharding import Mesh
from jax.sharding import PartitionSpec as P

AXES = ("zlo", "x", "core", "y", "zhi")
VOCAB = ("zlo", "x", "core")
SEQ = ("y", "zhi")

EARLY = (("z4", 0), ("x", 0), ("y", 0), ("z", 0))
ORDERS = ("xyz", "yzx", "zxy")
CUTS = (0, 6, 11, 16)
ROWS = 8
VMEM_LIMIT = 14 * 2**20


def pair(p, which, n):
    return jnp.where(which == 0, p ^ 1, (((p + 1) % n) ^ 1) + n - 1) % n


def partner(dim, ab, x, y, z, c):
    w = c ^ ab
    if dim == "x":
        return pair(x, w, 4), y, z
    if dim == "y":
        return x, pair(y, w, 4), z
    if dim == "z":
        return x, y, pair(z, w, 8)
    return x, y, z ^ 4


def linear(x, y, z, c):
    return ((((z % 4) * 4 + x) * 2 + c) * 4 + y) * 2 + z // 4


def stage_pairs(*stages):
    at = np.arange(256)
    zhi, y, c, x, zlo = at % 2, at // 2 % 4, at // 8 % 2, at // 16 % 4, at // 64
    z = zhi * 4 + zlo

    def ring(p, which, n):
        return np.where(which == 0, p ^ 1, (((p + 1) % n) ^ 1) + n - 1) % n

    for dim, ab in stages:
        w = c ^ ab
        if dim == "c":
            c = c ^ 1
        elif dim == "x":
            x = ring(x, w, 4)
        elif dim == "y":
            y = ring(y, w, 4)
        elif dim == "z":
            z = ring(z, w, 8)
        else:
            z = z ^ 4
    return tuple((int(a), int(b)) for a, b in zip(at, linear(x, y, z, c)))


def exchange(v, *stages):
    return lax.ppermute(v, AXES, stage_pairs(*stages))


def late(v, k, s):
    with jax.named_scope(f"late_{k}_{s}"):
        return exchange(v, (ORDERS[k][s], 1))


def normalize(rows, norm_gain):
    values = rows.astype(jnp.float32)
    meansq = jnp.mean(values * values, axis=-1, keepdims=True)
    return (values * lax.rsqrt(meansq + 1e-06) * norm_gain).astype(jnp.bfloat16)


def score_kernel(has_before, base_ref, tgt_ref, *refs):
    if has_before:
        before, *refs = refs
    *pieces, emb0, emb1, out_ref, turned, tot, pick = refs
    tot[...] = jnp.zeros_like(tot)
    pick[...] = jnp.zeros_like(pick)
    turned[...] = jnp.concatenate([piece[...] for piece in pieces], axis=0).T
    wide = turned.shape[1]
    for which, emb in enumerate((emb0, emb1)):
        count = emb.shape[0]
        for at in range(0, count, 256):
            tile = min(256, count - at)
            scores = jnp.dot(emb[at : at + tile], turned[...], preferred_element_type=jnp.float32)
            capped = 30.0 * jnp.tanh(scores * (1.0 / 30.0))
            grown = jnp.exp(capped)
            want = tgt_ref[...] - (base_ref[which] + at)
            ids = lax.broadcasted_iota(jnp.int32, scores.shape, 0)
            hit = jnp.where(ids == want, capped, 0.0)
            tot[...] += jnp.sum(grown.reshape(tile // 8, 8, wide), axis=0)
            pick[...] += jnp.sum(hit.reshape(tile // 8, 8, wide), axis=0)
    done = 0
    if has_before:
        done = before.shape[1]
        out_ref[:, :done] = before[...]
    out_ref[0:1, done:] = jnp.sum(tot[...], axis=0, keepdims=True)
    out_ref[1:2, done:] = jnp.sum(pick[...], axis=0, keepdims=True)


def score(pieces, emb0, emb1, bases, tgt, before=None):
    count, width = emb0.shape
    n = sum(p.shape[0] for p in pieces)
    vmem = pl.BlockSpec(memory_space=pltpu.VMEM)
    earlier = [] if before is None else [before]
    return pl.pallas_call(
        functools.partial(score_kernel, len(earlier)),
        out_shape=jax.ShapeDtypeStruct((2, n + sum(b.shape[1] for b in earlier)), jnp.float32),
        in_specs=[pl.BlockSpec(memory_space=pltpu.SMEM)] + [vmem] * (3 + len(earlier) + len(pieces)),
        out_specs=vmem,
        scratch_shapes=[
            pltpu.VMEM((width, n), jnp.bfloat16),
            pltpu.VMEM((8, n), jnp.float32),
            pltpu.VMEM((8, n), jnp.float32),
        ],
        compiler_params=pltpu.CompilerParams(vmem_limit_bytes=VMEM_LIMIT),
        cost_estimate=pl.CostEstimate(
            flops=4 * count * n * width,
            bytes_accessed=4 * count * width + 2 * n * width,
            transcendentals=4 * count * n,
        ),
        name="score",
    )(bases, tgt, *earlier, *pieces, emb0, emb1)


def load_kernel(src, dst, sems):
    part = dst.shape[0] // sems.shape[0]
    copies = [
        pltpu.make_async_copy(src.at[pl.ds(i * part, part)], dst.at[pl.ds(i * part, part)], sems.at[i])
        for i in range(sems.shape[0])
    ]
    for copy in copies:
        copy.start()
    for copy in copies:
        copy.wait()


def load(table):
    return pl.pallas_call(
        load_kernel,
        out_shape=jax.ShapeDtypeStruct(table.shape, table.dtype),
        in_specs=[pl.BlockSpec(memory_space=pltpu.HBM)],
        out_specs=pl.BlockSpec(memory_space=pltpu.VMEM),
        scratch_shapes=[pltpu.SemaphoreType.DMA((5,))],
        compiler_params=pltpu.CompilerParams(vmem_limit_bytes=43 * 2**20),
        cost_estimate=pl.CostEstimate(flops=3 * 10**8, bytes_accessed=2 * table.size, transcendentals=0),
        name="load",
    )(table)


def layout_of_rows():
    out = []
    for last in (0, 1):
        for l2 in (0, 1):
            for k in range(3):
                for l1 in (0, 1):
                    for e in range(CUTS[k], CUTS[k + 1]):
                        out.append((k, e, l1, l2, last))
    return np.array(out)


def sources():
    x, y, c = (lax.axis_index(a) for a in ("x", "y", "core"))
    z = lax.axis_index("zhi") * 4 + lax.axis_index("zlo")
    lay = layout_of_rows()
    n = len(lay)
    x, y, z = (jnp.full((n,), v, jnp.int32) for v in (x, y, z))

    def move(mask, dim, ab, x, y, z):
        mask = jnp.asarray(mask)
        return tuple(jnp.where(mask, a, b) for a, b in zip(partner(dim, ab, x, y, z, c), (x, y, z)))

    for s in (2, 1, 0):
        bit = lay[:, 2 + s] == 1
        dims = np.array([ORDERS[k][s] for k in lay[:, 0]])
        for dim in "xyz":
            x, y, z = move(bit & (dims == dim), dim, 1, x, y, z)
    for s in (3, 2, 1, 0):
        x, y, z = move((lay[:, 1] >> s) & 1 == 1, *EARLY[s], x, y, z)
    return x, y, z


def local(hidden_states, norm_gain, embedding, targets):
    all_count = targets.shape[0]
    block, part = hidden_states.shape
    core = lax.axis_index("core")
    y, zhi = lax.axis_index("y"), lax.axis_index("zhi")

    mine = ((lax.axis_index("zlo") * 4 + lax.axis_index("x")) * 2 * 8) + y * 2 + zhi
    bases = jnp.stack([mine + core * 8, mine + (1 - core) * 8]).astype(jnp.int32) * embedding.shape[0]

    sent = hidden_states.reshape(32, block // 32, part)
    came = lax.all_to_all(sent, VOCAB, split_axis=0, concat_axis=0, tiled=True)
    rows = jnp.moveaxis(came, 0, 1).reshape(block // 32, 32 * part)
    cur = normalize(rows, norm_gain)

    sx, sy, sz = sources()
    group = ((sy * 2 + sz // 4) * 4 + sz % 4) * 4 + sx
    tgt = jnp.take(targets.reshape(128, 2, ROWS), group, axis=0)
    tgt = jnp.where(core == 0, tgt[:, 0], tgt[:, 1]).reshape(2, 1, -1)
    tgt = list(tgt)

    cur, tgt, bases, embedding = lax.optimization_barrier((cur, tgt, bases, embedding))
    other = exchange(embedding, ("c", 0))
    own = load(embedding)

    for a in EARLY[:2]:
        came = exchange(cur, a)
        came, own = lax.optimization_barrier((came, own))
        cur = jnp.concatenate([cur, came], 0)
    a, b = EARLY[2:]
    cur = jnp.concatenate([cur, exchange(cur, a), exchange(cur, b), exchange(cur, a, b)], 0)
    groups = [cur[ROWS * a : ROWS * b] for a, b in zip(CUTS, CUTS[1:])]
    groups = [jnp.concatenate([g, late(g, k, 0)], 0) for k, g in enumerate(groups)]
    second = [late(g, k, 1) for k, g in enumerate(groups)]
    third = [late(g, k, 2) for k, g in enumerate(groups)]
    fourth = [late(g, k, 2) for k, g in enumerate(second)]

    stats = None
    for pieces, t in zip((groups + second, third + fourth), tgt):
        stats = score(pieces, own, other, bases, t, stats)
    stats = stats.reshape(2, -1, ROWS)
    order = (group[None, :] == jnp.arange(128, dtype=jnp.int32)[:, None]).astype(jnp.float32)
    stats = jnp.einsum("gp,spi->sgi", order, stats, precision=lax.Precision.HIGHEST)

    flat = jnp.broadcast_to(stats.reshape(1, 16, 128), (16, 16, 128))
    summed = lax.all_to_all(flat, ("x", "y"), split_axis=0, concat_axis=0, tiled=True).sum(axis=0, keepdims=True)
    flat = jnp.broadcast_to(summed, (16, 16, 128))
    got = lax.all_to_all(flat, ("core", "zhi", "zlo"), split_axis=0, concat_axis=0, tiled=True)
    total, picked = jnp.split(got.reshape(2, 8, 16, 128).sum(axis=1), 2, axis=1)
    loss = jnp.log(total) - picked
    mine = lax.dynamic_index_in_dim(loss, y * 2 + zhi, axis=1, keepdims=False)
    token_loss = jnp.moveaxis(mine.reshape(2, 16, ROWS), 0, 1).reshape(-1)
    return token_loss, jnp.sum(loss) / all_count


def solution(mesh):
    torus = Mesh(mesh.devices.reshape(4, 4, 2, 4, 2), AXES)
    placed = (P(SEQ, VOCAB), P(), P(VOCAB + SEQ, None), P())
    return jax.shard_map(
        local, mesh=torus, in_specs=placed, out_specs=(P(SEQ), P()), check_vma=False
    )
```

```python
import functools

import jax
import jax.numpy as jnp
import numpy as np
from jax import lax
from jax.experimental import pallas as pl
from jax.experimental.pallas import tpu as pltpu
from jax.sharding import Mesh
from jax.sharding import PartitionSpec as P

AXES = ("zlo", "x", "core", "y", "zhi")
VOCAB = ("zlo", "x", "core")
SEQ = ("y", "zhi")

EARLY = (("z4", 0), ("x", 0), ("y", 0), ("z", 0))
ORDERS = ("xyz", "yzx", "zxy")
CUTS = (0, 6, 11, 16)
ROWS = 8
VMEM_LIMIT = 14 * 2**20


def pair(p, which, n):
    return jnp.where(which == 0, p ^ 1, (((p + 1) % n) ^ 1) + n - 1) % n


def partner(dim, ab, x, y, z, c):
    w = c ^ ab
    if dim == "x":
        return pair(x, w, 4), y, z
    if dim == "y":
        return x, pair(y, w, 4), z
    if dim == "z":
        return x, y, pair(z, w, 8)
    return x, y, z ^ 4


def linear(x, y, z, c):
    return ((((z % 4) * 4 + x) * 2 + c) * 4 + y) * 2 + z // 4


def stage_pairs(*stages):
    at = np.arange(256)
    zhi, y, c, x, zlo = at % 2, at // 2 % 4, at // 8 % 2, at // 16 % 4, at // 64
    z = zhi * 4 + zlo

    def ring(p, which, n):
        return np.where(which == 0, p ^ 1, (((p + 1) % n) ^ 1) + n - 1) % n

    for dim, ab in stages:
        w = c ^ ab
        if dim == "c":
            c = c ^ 1
        elif dim == "x":
            x = ring(x, w, 4)
        elif dim == "y":
            y = ring(y, w, 4)
        elif dim == "z":
            z = ring(z, w, 8)
        else:
            z = z ^ 4
    return tuple((int(a), int(b)) for a, b in zip(at, linear(x, y, z, c)))


def exchange(v, *stages):
    return lax.ppermute(v, AXES, stage_pairs(*stages))


def late(v, k, s):
    with jax.named_scope(f"late_{k}_{s}"):
        return exchange(v, (ORDERS[k][s], 1))


def normalize(rows, norm_gain):
    values = rows.astype(jnp.float32)
    meansq = jnp.mean(values * values, axis=-1, keepdims=True)
    return (values * lax.rsqrt(meansq + 1e-06) * norm_gain).astype(jnp.bfloat16)


def score_kernel(has_before, base_ref, tgt_ref, *refs):
    if has_before:
        before, *refs = refs
    *pieces, emb0, emb1, out_ref, turned, tot, pick = refs
    tot[...] = jnp.zeros_like(tot)
    pick[...] = jnp.zeros_like(pick)
    turned[...] = jnp.concatenate([piece[...] for piece in pieces], axis=0).T
    wide = turned.shape[1]
    for which, emb in enumerate((emb0, emb1)):
        count = emb.shape[0]
        for at in range(0, count, 256):
            tile = min(256, count - at)
            scores = jnp.dot(emb[at : at + tile], turned[...], preferred_element_type=jnp.float32)
            capped = 30.0 * jnp.tanh(scores * (1.0 / 30.0))
            grown = jnp.exp(capped)
            want = tgt_ref[...] - (base_ref[which] + at)
            ids = lax.broadcasted_iota(jnp.int32, scores.shape, 0)
            hit = jnp.where(ids == want, capped, 0.0)
            tot[...] += jnp.sum(grown.reshape(tile // 8, 8, wide), axis=0)
            pick[...] += jnp.sum(hit.reshape(tile // 8, 8, wide), axis=0)
    done = 0
    if has_before:
        done = before.shape[1]
        out_ref[:, :done] = before[...]
    out_ref[0:1, done:] = jnp.sum(tot[...], axis=0, keepdims=True)
    out_ref[1:2, done:] = jnp.sum(pick[...], axis=0, keepdims=True)


def score(pieces, emb0, emb1, bases, tgt, before=None):
    count, width = emb0.shape
    n = sum(p.shape[0] for p in pieces)
    vmem = pl.BlockSpec(memory_space=pltpu.VMEM)
    earlier = [] if before is None else [before]
    return pl.pallas_call(
        functools.partial(score_kernel, len(earlier)),
        out_shape=jax.ShapeDtypeStruct((2, n + sum(b.shape[1] for b in earlier)), jnp.float32),
        in_specs=[pl.BlockSpec(memory_space=pltpu.SMEM)] + [vmem] * (3 + len(earlier) + len(pieces)),
        out_specs=vmem,
        scratch_shapes=[
            pltpu.VMEM((width, n), jnp.bfloat16),
            pltpu.VMEM((8, n), jnp.float32),
            pltpu.VMEM((8, n), jnp.float32),
        ],
        compiler_params=pltpu.CompilerParams(vmem_limit_bytes=VMEM_LIMIT),
        cost_estimate=pl.CostEstimate(
            flops=4 * count * n * width,
            bytes_accessed=4 * count * width + 2 * n * width,
            transcendentals=4 * count * n,
        ),
        name="score",
    )(bases, tgt, *earlier, *pieces, emb0, emb1)


def rows_of(parts, start, stop):
    out, at = [], 0
    for part in parts:
        n = part.shape[0]
        if start < at + n and at < stop:
            out.append(part[max(start - at, 0) : min(stop - at, n)])
        at += n
    return lax.optimization_barrier(jnp.concatenate(out, 0))


def load_kernel(src, dst, sems):
    part = dst.shape[0] // sems.shape[0]
    copies = [
        pltpu.make_async_copy(src.at[pl.ds(i * part, part)], dst.at[pl.ds(i * part, part)], sems.at[i])
        for i in range(sems.shape[0])
    ]
    for copy in copies:
        copy.start()
    for copy in copies:
        copy.wait()


def load(table):
    return pl.pallas_call(
        load_kernel,
        out_shape=jax.ShapeDtypeStruct(table.shape, table.dtype),
        in_specs=[pl.BlockSpec(memory_space=pltpu.HBM)],
        out_specs=pl.BlockSpec(memory_space=pltpu.VMEM),
        scratch_shapes=[pltpu.SemaphoreType.DMA((5,))],
        compiler_params=pltpu.CompilerParams(vmem_limit_bytes=43 * 2**20),
        cost_estimate=pl.CostEstimate(flops=3 * 10**8, bytes_accessed=2 * table.size, transcendentals=0),
        name="load",
    )(table)


def layout_of_rows():
    out = []
    for last in (0, 1):
        for l2 in (0, 1):
            for k in range(3):
                for l1 in (0, 1):
                    for e in range(CUTS[k], CUTS[k + 1]):
                        out.append((k, e, l1, l2, last))
    return np.array(out)


def sources():
    x, y, c = (lax.axis_index(a) for a in ("x", "y", "core"))
    z = lax.axis_index("zhi") * 4 + lax.axis_index("zlo")
    lay = layout_of_rows()
    n = len(lay)
    x, y, z = (jnp.full((n,), v, jnp.int32) for v in (x, y, z))

    def move(mask, dim, ab, x, y, z):
        mask = jnp.asarray(mask)
        return tuple(jnp.where(mask, a, b) for a, b in zip(partner(dim, ab, x, y, z, c), (x, y, z)))

    for s in (2, 1, 0):
        bit = lay[:, 2 + s] == 1
        dims = np.array([ORDERS[k][s] for k in lay[:, 0]])
        for dim in "xyz":
            x, y, z = move(bit & (dims == dim), dim, 1, x, y, z)
    for s in (3, 2, 1, 0):
        x, y, z = move((lay[:, 1] >> s) & 1 == 1, *EARLY[s], x, y, z)
    return x, y, z


def local(hidden_states, norm_gain, embedding, targets):
    all_count = targets.shape[0]
    block, part = hidden_states.shape
    core = lax.axis_index("core")
    y, zhi = lax.axis_index("y"), lax.axis_index("zhi")

    mine = ((lax.axis_index("zlo") * 4 + lax.axis_index("x")) * 2 * 8) + y * 2 + zhi
    bases = jnp.stack([mine + core * 8, mine + (1 - core) * 8]).astype(jnp.int32) * embedding.shape[0]

    sent = hidden_states.reshape(32, block // 32, part)
    came = lax.all_to_all(sent, VOCAB, split_axis=0, concat_axis=0, tiled=True)
    rows = jnp.moveaxis(came, 0, 1).reshape(block // 32, 32 * part)
    cur = normalize(rows, norm_gain)

    sx, sy, sz = sources()
    group = ((sy * 2 + sz // 4) * 4 + sz % 4) * 4 + sx
    tgt = jnp.take(targets.reshape(128, 2, ROWS), group, axis=0)
    tgt = jnp.where(core == 0, tgt[:, 0], tgt[:, 1]).reshape(4, 1, -1)
    tgt = list(tgt)

    cur, tgt, bases, embedding = lax.optimization_barrier((cur, tgt, bases, embedding))
    other = exchange(embedding, ("c", 0))
    own = load(embedding)

    for a in EARLY[:2]:
        came = exchange(cur, a)
        came, own = lax.optimization_barrier((came, own))
        cur = jnp.concatenate([cur, came], 0)
    a, b = EARLY[2:]
    parts = [cur, exchange(cur, a), exchange(cur, b), exchange(cur, a, b)]
    groups = [rows_of(parts, ROWS * a, ROWS * b) for a, b in zip(CUTS, CUTS[1:])]
    groups = [jnp.concatenate([g, late(g, k, 0)], 0) for k, g in enumerate(groups)]
    second = [late(g, k, 1) for k, g in enumerate(groups)]
    third = [late(g, k, 2) for k, g in enumerate(groups)]
    stats = score(groups, own, other, bases, tgt[0])
    stats, second = lax.optimization_barrier((stats, second))
    fourth = [late(g, k, 2) for k, g in enumerate(second)]
    for pieces, t in zip((second, third, fourth), tgt[1:]):
        stats = score(pieces, own, other, bases, t, stats)
    stats = stats.reshape(2, -1, ROWS)
    order = (group[None, :] == jnp.arange(128, dtype=jnp.int32)[:, None]).astype(jnp.float32)
    stats = jnp.einsum("gp,spi->sgi", order, stats, precision=lax.Precision.HIGHEST)

    flat = jnp.broadcast_to(stats.reshape(1, 16, 128), (16, 16, 128))
    summed = lax.all_to_all(flat, ("x", "y"), split_axis=0, concat_axis=0, tiled=True).sum(axis=0, keepdims=True)
    flat = jnp.broadcast_to(summed, (16, 16, 128))
    got = lax.all_to_all(flat, ("core", "zhi", "zlo"), split_axis=0, concat_axis=0, tiled=True)
    total, picked = jnp.split(got.reshape(2, 8, 16, 128).sum(axis=1), 2, axis=1)
    loss = jnp.log(total) - picked
    mine = lax.dynamic_index_in_dim(loss, y * 2 + zhi, axis=1, keepdims=False)
    token_loss = jnp.moveaxis(mine.reshape(2, 16, ROWS), 0, 1).reshape(-1)
    return token_loss, jnp.sum(loss) / all_count


def solution(mesh):
    torus = Mesh(mesh.devices.reshape(4, 4, 2, 4, 2), AXES)
    placed = (P(SEQ, VOCAB), P(), P(VOCAB + SEQ, None), P())
    return jax.shard_map(
        local, mesh=torus, in_specs=placed, out_specs=(P(SEQ), P()), check_vma=False
    )
```

```python
import functools

import jax
import jax.numpy as jnp
import numpy as np
from jax import lax
from jax.experimental import pallas as pl
from jax.experimental.pallas import tpu as pltpu
from jax.sharding import Mesh
from jax.sharding import PartitionSpec as P

AXES = ("zlo", "x", "core", "y", "zhi")
VOCAB = ("zlo", "x", "core")
SEQ = ("y", "zhi")

EARLY = (("z4", 0), ("x", 0), ("y", 0), ("z", 0))
ORDERS = ("xzy", "yxz", "zyx")
CUTS = (0, 6, 11, 16)
ROWS = 8
VMEM_LIMIT = 14 * 2**20


def pair(p, which, n):
    return jnp.where(which == 0, p ^ 1, (((p + 1) % n) ^ 1) + n - 1) % n


def partner(dim, ab, x, y, z, c):
    w = c ^ ab
    if dim == "x":
        return pair(x, w, 4), y, z
    if dim == "y":
        return x, pair(y, w, 4), z
    if dim == "z":
        return x, y, pair(z, w, 8)
    return x, y, z ^ 4


def linear(x, y, z, c):
    return ((((z % 4) * 4 + x) * 2 + c) * 4 + y) * 2 + z // 4


def stage_pairs(*stages):
    at = np.arange(256)
    zhi, y, c, x, zlo = at % 2, at // 2 % 4, at // 8 % 2, at // 16 % 4, at // 64
    z = zhi * 4 + zlo

    def ring(p, which, n):
        return np.where(which == 0, p ^ 1, (((p + 1) % n) ^ 1) + n - 1) % n

    for dim, ab in stages:
        w = c ^ ab
        if dim == "c":
            c = c ^ 1
        elif dim == "x":
            x = ring(x, w, 4)
        elif dim == "y":
            y = ring(y, w, 4)
        elif dim == "z":
            z = ring(z, w, 8)
        else:
            z = z ^ 4
    return tuple((int(a), int(b)) for a, b in zip(at, linear(x, y, z, c)))


def exchange(v, *stages):
    return lax.ppermute(v, AXES, stage_pairs(*stages))


def late(v, k, s):
    with jax.named_scope(f"late_{k}_{s}"):
        return exchange(v, (ORDERS[k][s], 1))


def normalize(rows, norm_gain):
    values = rows.astype(jnp.float32)
    meansq = jnp.mean(values * values, axis=-1, keepdims=True)
    return (values * lax.rsqrt(meansq + 1e-06) * norm_gain).astype(jnp.bfloat16)


def score_kernel(has_before, base_ref, tgt_ref, *refs):
    if has_before:
        before, *refs = refs
    *pieces, emb0, emb1, out_ref, turned, tot, pick = refs
    tot[...] = jnp.zeros_like(tot)
    pick[...] = jnp.zeros_like(pick)
    turned[...] = jnp.concatenate([piece[...] for piece in pieces], axis=0).T
    wide = turned.shape[1]
    for which, emb in enumerate((emb0, emb1)):
        count = emb.shape[0]
        for at in range(0, count, 256):
            tile = min(256, count - at)
            scores = jnp.dot(emb[at : at + tile], turned[...], preferred_element_type=jnp.float32)
            capped = 30.0 * jnp.tanh(scores * (1.0 / 30.0))
            grown = jnp.exp(capped)
            want = tgt_ref[...] - (base_ref[which] + at)
            ids = lax.broadcasted_iota(jnp.int32, scores.shape, 0)
            hit = jnp.where(ids == want, capped, 0.0)
            tot[...] += jnp.sum(grown.reshape(tile // 8, 8, wide), axis=0)
            pick[...] += jnp.sum(hit.reshape(tile // 8, 8, wide), axis=0)
    done = 0
    if has_before:
        done = before.shape[1]
        out_ref[:, :done] = before[...]
    out_ref[0:1, done:] = jnp.sum(tot[...], axis=0, keepdims=True)
    out_ref[1:2, done:] = jnp.sum(pick[...], axis=0, keepdims=True)


def score(pieces, emb0, emb1, bases, tgt, before=None):
    count, width = emb0.shape
    n = sum(p.shape[0] for p in pieces)
    vmem = pl.BlockSpec(memory_space=pltpu.VMEM)
    earlier = [] if before is None else [before]
    return pl.pallas_call(
        functools.partial(score_kernel, len(earlier)),
        out_shape=jax.ShapeDtypeStruct((2, n + sum(b.shape[1] for b in earlier)), jnp.float32),
        in_specs=[pl.BlockSpec(memory_space=pltpu.SMEM)] + [vmem] * (3 + len(earlier) + len(pieces)),
        out_specs=vmem,
        scratch_shapes=[
            pltpu.VMEM((width, n), jnp.bfloat16),
            pltpu.VMEM((8, n), jnp.float32),
            pltpu.VMEM((8, n), jnp.float32),
        ],
        compiler_params=pltpu.CompilerParams(vmem_limit_bytes=VMEM_LIMIT),
        cost_estimate=pl.CostEstimate(
            flops=4 * count * n * width,
            bytes_accessed=4 * count * width + 2 * n * width,
            transcendentals=4 * count * n,
        ),
        name="score",
    )(bases, tgt, *earlier, *pieces, emb0, emb1)


def rows_of(parts, start, stop):
    out, at = [], 0
    for part in parts:
        n = part.shape[0]
        if start < at + n and at < stop:
            out.append(part[max(start - at, 0) : min(stop - at, n)])
        at += n
    return lax.optimization_barrier(jnp.concatenate(out, 0))


def load_kernel(src, dst, sems):
    part = dst.shape[0] // sems.shape[0]
    copies = [
        pltpu.make_async_copy(src.at[pl.ds(i * part, part)], dst.at[pl.ds(i * part, part)], sems.at[i])
        for i in range(sems.shape[0])
    ]
    for copy in copies:
        copy.start()
    for copy in copies:
        copy.wait()


def load(table):
    return pl.pallas_call(
        load_kernel,
        out_shape=jax.ShapeDtypeStruct(table.shape, table.dtype),
        in_specs=[pl.BlockSpec(memory_space=pltpu.HBM)],
        out_specs=pl.BlockSpec(memory_space=pltpu.VMEM),
        scratch_shapes=[pltpu.SemaphoreType.DMA((5,))],
        compiler_params=pltpu.CompilerParams(vmem_limit_bytes=43 * 2**20),
        cost_estimate=pl.CostEstimate(flops=3 * 10**8, bytes_accessed=2 * table.size, transcendentals=0),
        name="load",
    )(table)


def layout_of_rows():
    out = []
    for last in (0, 1):
        for l2 in (0, 1):
            for k in range(3):
                for l1 in (0, 1):
                    for e in range(CUTS[k], CUTS[k + 1]):
                        out.append((k, e, l1, l2, last))
    return np.array(out)


def sources():
    x, y, c = (lax.axis_index(a) for a in ("x", "y", "core"))
    z = lax.axis_index("zhi") * 4 + lax.axis_index("zlo")
    lay = layout_of_rows()
    n = len(lay)
    x, y, z = (jnp.full((n,), v, jnp.int32) for v in (x, y, z))

    def move(mask, dim, ab, x, y, z):
        mask = jnp.asarray(mask)
        return tuple(jnp.where(mask, a, b) for a, b in zip(partner(dim, ab, x, y, z, c), (x, y, z)))

    for s in (2, 1, 0):
        bit = lay[:, 2 + s] == 1
        dims = np.array([ORDERS[k][s] for k in lay[:, 0]])
        for dim in "xyz":
            x, y, z = move(bit & (dims == dim), dim, 1, x, y, z)
    for s in (3, 2, 1, 0):
        x, y, z = move((lay[:, 1] >> s) & 1 == 1, *EARLY[s], x, y, z)
    return x, y, z


def local(hidden_states, norm_gain, embedding, targets):
    all_count = targets.shape[0]
    block, part = hidden_states.shape
    core = lax.axis_index("core")
    y, zhi = lax.axis_index("y"), lax.axis_index("zhi")

    mine = ((lax.axis_index("zlo") * 4 + lax.axis_index("x")) * 2 * 8) + y * 2 + zhi
    bases = jnp.stack([mine + core * 8, mine + (1 - core) * 8]).astype(jnp.int32) * embedding.shape[0]

    sent = hidden_states.reshape(32, block // 32, part)
    came = lax.all_to_all(sent, VOCAB, split_axis=0, concat_axis=0, tiled=True)
    rows = jnp.moveaxis(came, 0, 1).reshape(block // 32, 32 * part)
    cur = normalize(rows, norm_gain)

    sx, sy, sz = sources()
    group = ((sy * 2 + sz // 4) * 4 + sz % 4) * 4 + sx
    tgt = jnp.take(targets.reshape(128, 2, ROWS), group, axis=0)
    tgt = jnp.where(core == 0, tgt[:, 0], tgt[:, 1]).reshape(4, 1, -1)
    tgt = list(tgt)

    cur, tgt, bases, embedding = lax.optimization_barrier((cur, tgt, bases, embedding))
    other = exchange(embedding, ("c", 0))
    own = load(embedding)

    for a in EARLY[:2]:
        came = exchange(cur, a)
        came, own = lax.optimization_barrier((came, own))
        cur = jnp.concatenate([cur, came], 0)
    a, b = EARLY[2:]
    parts = [cur, exchange(cur, a), exchange(cur, b), exchange(cur, a, b)]
    groups = [rows_of(parts, ROWS * a, ROWS * b) for a, b in zip(CUTS, CUTS[1:])]
    groups = [jnp.concatenate([g, late(g, k, 0)], 0) for k, g in enumerate(groups)]
    second = [late(g, k, 1) for k, g in enumerate(groups)]
    third = [late(g, k, 2) for k, g in enumerate(groups)]
    stats = score(groups, own, other, bases, tgt[0])
    stats, second = lax.optimization_barrier((stats, second))
    fourth = [late(g, k, 2) for k, g in enumerate(second)]
    for pieces, t in zip((second, third, fourth), tgt[1:]):
        stats = score(pieces, own, other, bases, t, stats)
    stats = stats.reshape(2, -1, ROWS)
    order = (group[None, :] == jnp.arange(128, dtype=jnp.int32)[:, None]).astype(jnp.float32)
    stats = jnp.einsum("gp,spi->sgi", order, stats, precision=lax.Precision.HIGHEST)

    flat = jnp.broadcast_to(stats.reshape(1, 16, 128), (16, 16, 128))
    summed = lax.all_to_all(flat, ("x", "y"), split_axis=0, concat_axis=0, tiled=True).sum(axis=0, keepdims=True)
    flat = jnp.broadcast_to(summed, (16, 16, 128))
    got = lax.all_to_all(flat, ("core", "zhi", "zlo"), split_axis=0, concat_axis=0, tiled=True)
    total, picked = jnp.split(got.reshape(2, 8, 16, 128).sum(axis=1), 2, axis=1)
    loss = jnp.log(total) - picked
    mine = lax.dynamic_index_in_dim(loss, y * 2 + zhi, axis=1, keepdims=False)
    token_loss = jnp.moveaxis(mine.reshape(2, 16, ROWS), 0, 1).reshape(-1)
    return token_loss, jnp.sum(loss) / all_count


def solution(mesh):
    torus = Mesh(mesh.devices.reshape(4, 4, 2, 4, 2), AXES)
    placed = (P(SEQ, VOCAB), P(), P(VOCAB + SEQ, None), P())
    return jax.shard_map(
        local, mesh=torus, in_specs=placed, out_specs=(P(SEQ), P()), check_vma=False
    )
```
